16 devices in a mesh: dp: 2 (over z), sp: 8 (over y, x, core).
Axes of the slice: x: 2, y: 2, z: 2, core: 2. Of those that a mesh axis runs over, the one named last changes fastest.
Arguments:
- hidden: bfloat16 [16, 2048, 2048], P('dp', 'sp'), parts along dimension 0
- grad_out: bfloat16 [16, 2048, 2048], P('dp', 'sp'), parts along dimension 0
- w_query: bfloat16 [2048, 16, 128], replicated
- w_key: bfloat16 [2048, 128], replicated
- w_value: bfloat16 [2048, 128], replicated
- w_out: bfloat16 [16, 128, 2048], replicated
Outputs:
- output 1: bfloat16 [16, 2048, 2048], P('dp', 'sp'), parts along dimension 0
- output 2: bfloat16 [16, 2048, 2048], P('dp', 'sp'), parts along dimension 0
- output 3: float32 [4096, 16, 128], P('dp'), parts along dimension 0
- output 4: float32 [4096, 128], P('dp'), parts along dimension 0
- output 5: float32 [4096, 128], P('dp'), parts along dimension 0
- output 6: float32 [32, 128, 2048], P('dp'), parts along dimension 0
There are 2 independent parts. The reference program is written for one: setup_inputs(seed, part) draws one part's arguments, and reference() takes and returns one part's arrays. A program takes and returns all parts, laid end to end along the dimension named above; an argument that names none is the same for every part.
All inputs are finite; a program needn't handle non-finite values.
Results may differ from the reference program's by a relative error of at most 0.02.
Values are sent between devices in bfloat16 or wider.
A program may use at most 1 GiB of HBM per device.

```python
import jax
import jax.numpy as jnp
from jax import lax

BATCH_PART = 8
SEQ_LEN = 2048
D_MODEL = 2048
N_HEADS = 16
HEAD_DIM = 128
QUERY_ROWS = min(SEQ_LEN, 128)
ROPE_BASE = 10000.0
NEG_BIG = -1e30


def setup_inputs(seed: int = 0, part: int = 0) -> dict:
    part_keys = jax.random.split(jax.random.fold_in(jax.random.key(seed), part), 2)
    weight_keys = jax.random.split(jax.random.key(seed + 1), 4)
    act_shape = (BATCH_PART, SEQ_LEN, D_MODEL)
    hidden = jax.random.normal(part_keys[0], act_shape, jnp.float32)
    grad_out = jax.random.normal(part_keys[1], act_shape, jnp.float32)
    w_query = jax.random.normal(weight_keys[0], (D_MODEL, N_HEADS, HEAD_DIM), jnp.float32) * D_MODEL ** -0.5
    w_key = jax.random.normal(weight_keys[1], (D_MODEL, HEAD_DIM), jnp.float32) * D_MODEL ** -0.5
    w_value = jax.random.normal(weight_keys[2], (D_MODEL, HEAD_DIM), jnp.float32) * D_MODEL ** -0.5
    w_out = jax.random.normal(weight_keys[3], (N_HEADS, HEAD_DIM, D_MODEL), jnp.float32) * (N_HEADS * HEAD_DIM) ** -0.5
    return {'hidden': hidden.astype(jnp.bfloat16), 'grad_out': grad_out.astype(jnp.bfloat16), 'w_query': w_query.astype(jnp.bfloat16), 'w_key': w_key.astype(jnp.bfloat16), 'w_value': w_value.astype(jnp.bfloat16), 'w_out': w_out.astype(jnp.bfloat16)}


def rope_tables(positions):
    half_dim = HEAD_DIM // 2
    inv_freq = ROPE_BASE ** (-jnp.arange(half_dim, dtype=jnp.float32) * (2.0 / HEAD_DIM))
    angles = positions.astype(jnp.float32)[:, None] * inv_freq[None, :]
    return jnp.cos(angles), jnp.sin(angles)


def rotate(x_in, cos_t, sin_t):
    half_dim = x_in.shape[-1] // 2
    lead_half = x_in[..., :half_dim]
    tail_half = x_in[..., half_dim:]
    return jnp.concatenate([lead_half * cos_t - tail_half * sin_t, tail_half * cos_t + lead_half * sin_t], axis=-1)


def to_bf16(x_in):
    return x_in + lax.stop_gradient(x_in.astype(jnp.bfloat16).astype(jnp.float32) - x_in)


def block_attend(q_blk, row_start, k_rot, v_proj):
    scores = jnp.einsum('bqhe,bke->bhqk', q_blk, k_rot)
    row_ids = row_start + jnp.arange(QUERY_ROWS)
    col_ids = jnp.arange(SEQ_LEN)
    scores = jnp.where(col_ids[None, :] <= row_ids[:, None], scores, NEG_BIG)
    attn_probs = to_bf16(jax.nn.softmax(scores, axis=-1))
    return to_bf16(jnp.einsum('bhqk,bke->bqhe', attn_probs, v_proj))


def forward(hidden, w_query, w_key, w_value, w_out):
    cos_t, sin_t = rope_tables(jnp.arange(SEQ_LEN))
    queries = to_bf16(jnp.einsum('bsd,dhe->bshe', hidden, w_query))
    key_proj = to_bf16(jnp.einsum('bsd,de->bse', hidden, w_key))
    val_proj = to_bf16(jnp.einsum('bsd,de->bse', hidden, w_value))
    q_rot = to_bf16(rotate(queries * HEAD_DIM ** -0.5, cos_t[:, None, :], sin_t[:, None, :]))
    k_rot = to_bf16(rotate(key_proj, cos_t, sin_t))
    n_blocks = SEQ_LEN // QUERY_ROWS
    q_blocks = jnp.moveaxis(q_rot.reshape(BATCH_PART, n_blocks, QUERY_ROWS, N_HEADS, HEAD_DIM), 1, 0)
    attend = jax.checkpoint(block_attend)
    o_blocks = lax.map(lambda block_pair: attend(block_pair[0], block_pair[1], k_rot, val_proj), (q_blocks, jnp.arange(n_blocks) * QUERY_ROWS))
    o_heads = jnp.moveaxis(o_blocks, 0, 1).reshape(BATCH_PART, SEQ_LEN, N_HEADS, HEAD_DIM)
    return to_bf16(jnp.einsum('bshe,hed->bsd', o_heads, w_out))


def reference(hidden, grad_out, w_query, w_key, w_value, w_out):
    attn_out, pullback = jax.vjp(forward, hidden.astype(jnp.float32), w_query.astype(jnp.float32), w_key.astype(jnp.float32), w_value.astype(jnp.float32), w_out.astype(jnp.float32))
    d_hidden, dw_query, dw_key, dw_value, dw_out = pullback(grad_out.astype(jnp.float32))
    return (attn_out.astype(jnp.bfloat16), d_hidden.astype(jnp.bfloat16), dw_query, dw_key, dw_value, dw_out)
```

```python
import functools

import jax
import jax.numpy as jnp
from jax import lax
from jax.experimental import pallas as pl
from jax.experimental.pallas import tpu as pltpu
from jax.sharding import PartitionSpec as P

ROPE_BASE = 10000.0
NEG_BIG = -1e30
HEADS_PER_GROUP = 4
NT = (((1,), (1,)), ((), ()))
NN = (((1,), (0,)), ((), ()))


def dot(a, b, dims):
    return lax.dot_general(a, b, dims, preferred_element_type=jnp.float32)


def rope_tables(positions, head_dim):
    half_dim = head_dim // 2
    inv_freq = ROPE_BASE ** (-jnp.arange(half_dim, dtype=jnp.float32) * (2.0 / head_dim))
    angles = positions.astype(jnp.float32)[:, None] * inv_freq[None, :]
    cos_t, sin_t = jnp.cos(angles), jnp.sin(angles)
    return jnp.concatenate([cos_t, cos_t], -1), jnp.concatenate([-sin_t, sin_t], -1)


def swap_halves(x):
    half = x.shape[-1] // 2
    return jnp.concatenate([x[..., half:], x[..., :half]], axis=-1)


def attn_kernel(heads, first, blk_ref, q_ref, do_ref, kv_ref, kvt_ref, cos_ref, sin_ref, *rest):
    if first:
        o_ref, dq_ref, dkv_ref, q_s, do_s, s_s, ot_s, dqt_s, p_s, ds_s, dp_s = rest
    else:
        dkv_in_ref, o_ref, dq_ref, dkv_ref, q_s, do_s, s_s, ot_s, dqt_s, p_s, ds_s, dp_s = rest
    me = blk_ref[0]
    rows, hd = cos_ref.shape
    n_blk = kv_ref.shape[0]
    keys = kv_ref.shape[2]
    width = heads * rows
    scale = hd ** -0.5
    cos2, sin2 = cos_ref[...], sin_ref[...]
    do_t = []
    for h in range(heads):
        q_h = q_ref[0, :, h * hd:(h + 1) * hd].astype(jnp.float32) * scale
        q_s[h * rows:(h + 1) * rows, :] = (q_h * cos2 + swap_halves(q_h) * sin2).astype(jnp.bfloat16)
        do_s[h * rows:(h + 1) * rows, :] = do_ref[0, :, h * hd:(h + 1) * hd]

    def score_block(kb, mask, m8):
        k_blk = kv_ref[kb, 0, :, :hd]
        out = []
        for h in range(heads):
            s = dot(k_blk, q_s[h * rows:(h + 1) * rows, :], NT)
            if mask is not None:
                s = jnp.where(mask, s, NEG_BIG)
            s_s[kb, :, h * rows:(h + 1) * rows] = s
            out.append(jnp.max(s.reshape(keys // 8, 8, rows), axis=0))
        return jnp.maximum(m8, jnp.concatenate(out, axis=1))

    m8 = lax.fori_loop(0, me, lambda kb, m: score_block(kb, None, m), jnp.full((8, width), NEG_BIG, jnp.float32))
    causal = lax.broadcasted_iota(jnp.int32, (keys, rows), 0) <= lax.broadcasted_iota(jnp.int32, (keys, rows), 1)
    m8 = score_block(me, causal, m8)
    m = jnp.max(m8, axis=0, keepdims=True)

    ot_s[...] = jnp.zeros_like(ot_s)
    dqt_s[...] = jnp.zeros_like(dqt_s)

    def weigh_values(kb):
        vt = kvt_ref[kb, 0, hd:, :]
        for h in range(heads):
            cols = slice(h * rows, (h + 1) * rows)
            ot_s[:, cols] += dot(vt, p_s[:, cols], NN)

    def value_block(kb, l8):
        weigh_values(jnp.maximum(kb - 1, 0))
        out = []
        for h in range(heads):
            cols = slice(h * rows, (h + 1) * rows)
            e = jnp.exp(s_s[kb, :, cols] - m[:, cols])
            s_s[kb, :, cols] = e
            out.append(jnp.sum(e.reshape(keys // 8, 8, rows), axis=0))
            p_s[:, cols] = e.astype(jnp.bfloat16)
        return l8 + jnp.concatenate(out, axis=1)

    p_s[...] = jnp.zeros_like(p_s)
    ds_s[...] = jnp.zeros_like(ds_s)
    l8 = lax.fori_loop(0, me + 1, value_block, jnp.zeros((8, width), jnp.float32))
    weigh_values(me)
    p_s[...] = jnp.zeros_like(p_s)
    rl = 1.0 / jnp.sum(l8, axis=0, keepdims=True)
    row_dot = []
    for h in range(heads):
        cols = slice(h * rows, (h + 1) * rows)
        o_t = (ot_s[:, cols] * rl[:, cols]).astype(jnp.bfloat16)
        o_ref[0, :, h * hd:(h + 1) * hd] = o_t.T
        do_t = do_ref[0, :, h * hd:(h + 1) * hd].T
        row_dot.append(jnp.sum(do_t.astype(jnp.float32) * o_t.astype(jnp.float32), axis=0, keepdims=True))
    row_dot = jnp.concatenate(row_dot, axis=1)

    def prob_grads(kb):
        v_blk = kv_ref[kb, 0, :, hd:]
        for h in range(heads):
            cols = slice(h * rows, (h + 1) * rows)
            dp_s[:, cols] = dot(v_blk, do_s[cols, :], NT)

    def products(kb):
        kt = kvt_ref[kb, 0, :hd, :]
        for h in range(heads):
            cols = slice(h * rows, (h + 1) * rows)
            dqt_s[:, cols] += dot(kt, ds_s[:, cols], NN)
        dkv = jnp.concatenate([dot(ds_s[...], q_s[...], NN), dot(p_s[...], do_s[...], NN)], axis=1)
        if not first:
            dkv = dkv + dkv_in_ref[kb, 0]
        dkv_ref[kb, 0] = dkv

    def grad_block(kb, _):
        products(jnp.maximum(kb - 1, 0))
        for h in range(heads):
            cols = slice(h * rows, (h + 1) * rows)
            p = s_s[kb, :, cols] * rl[:, cols]
            ds_s[:, cols] = (p * (dp_s[:, cols] - row_dot[:, cols])).astype(jnp.bfloat16)
            p_s[:, cols] = p.astype(jnp.bfloat16)
        prob_grads(jnp.minimum(kb + 1, me))
        return 0

    prob_grads(0)
    lax.fori_loop(0, me + 1, grad_block, 0)
    products(me)

    def zero_block(kb, _):
        dkv_ref[kb, 0] = jnp.zeros((keys, 2 * hd), jnp.float32)
        return 0

    lax.fori_loop(me + 1, n_blk, zero_block, 0)
    for h in range(heads):
        cols = slice(h * rows, (h + 1) * rows)
        g = dqt_s[:, cols].T
        dq_ref[0, :, h * hd:(h + 1) * hd] = ((g * cos2 - swap_halves(g) * sin2) * scale).astype(jnp.bfloat16)


def attend(group, heads, me, q, do, kv, kvt, cos2, sin2, dkv):
    n_batch, rows, _ = q.shape
    n_blk, _, keys, two_hd = kv.shape
    hd = two_hd // 2
    first = dkv is None
    width = heads * hd
    head_spec = pl.BlockSpec((1, rows, width), lambda b, s: (b, 0, group))
    kv_spec = pl.BlockSpec((n_blk, 1, keys, two_hd), lambda b, s: (0, b, 0, 0))
    kvt_spec = pl.BlockSpec((n_blk, 1, two_hd, keys), lambda b, s: (0, b, 0, 0))
    tab_spec = pl.BlockSpec((rows, hd), lambda b, s: (0, 0))
    out_spec = pl.BlockSpec((1, rows, width), lambda b, s: (b, 0, 0))
    in_specs = [head_spec, head_spec, kv_spec, kvt_spec, tab_spec, tab_spec]
    operands = [me, q, do, kv, kvt, cos2, sin2]
    aliases = {}
    if not first:
        in_specs.append(kv_spec)
        operands.append(dkv)
        aliases = {7: 2}
    flops = 12 * n_batch * heads * rows * keys * n_blk * hd
    return pl.pallas_call(
        functools.partial(attn_kernel, heads, first),
        grid_spec=pltpu.PrefetchScalarGridSpec(
            num_scalar_prefetch=1,
            grid=(n_batch,),
            in_specs=in_specs,
            out_specs=[out_spec, out_spec, kv_spec],
            scratch_shapes=[
                pltpu.VMEM((heads * rows, hd), jnp.bfloat16),
                pltpu.VMEM((heads * rows, hd), jnp.bfloat16),
                pltpu.VMEM((n_blk, keys, heads * rows), jnp.float32),
                pltpu.VMEM((hd, heads * rows), jnp.float32),
                pltpu.VMEM((hd, heads * rows), jnp.float32),
                pltpu.VMEM((keys, heads * rows), jnp.bfloat16),
                pltpu.VMEM((keys, heads * rows), jnp.bfloat16),
                pltpu.VMEM((keys, heads * rows), jnp.float32),
            ],
        ),
        out_shape=[
            jax.ShapeDtypeStruct((n_batch, rows, width), jnp.bfloat16),
            jax.ShapeDtypeStruct((n_batch, rows, width), jnp.bfloat16),
            jax.ShapeDtypeStruct((n_blk, n_batch, keys, two_hd), jnp.float32),
        ],
        input_output_aliases=aliases,
        compiler_params=pltpu.CompilerParams(vmem_limit_bytes=48 * 1024 * 1024),
        cost_estimate=pl.CostEstimate(flops=2 * flops, bytes_accessed=40_000_000, transcendentals=n_batch * heads * rows * keys * n_blk),
    )(*operands)


def solution(mesh):
    n_sp = mesh.shape['sp']

    def local_step(hid_loc, gout_loc, w_query, w_key, w_value, w_out):
        n_batch, seq_loc, d_model = hid_loc.shape
        n_heads, head_dim = w_query.shape[1:]
        full = n_heads * head_dim
        n_rows = n_batch * seq_loc
        me = lax.axis_index('sp')
        cos2, sin2 = rope_tables(me * seq_loc + jnp.arange(seq_loc), head_dim)
        w_kv = jnp.concatenate([w_key, w_value], axis=1)
        hid = hid_loc.reshape(n_rows, d_model)
        gout = gout_loc.reshape(n_rows, d_model)
        wo = w_out.reshape(full, d_model)
        kv = dot(hid, w_kv, NN).astype(jnp.bfloat16).reshape(n_batch, seq_loc, 2 * head_dim)
        k_f = kv[..., :head_dim].astype(jnp.float32)
        k_rot = (k_f * cos2 + swap_halves(k_f) * sin2).astype(jnp.bfloat16)
        kv = jnp.concatenate([k_rot, kv[..., head_dim:]], axis=-1)
        kv_all = lax.all_gather(kv, 'sp', axis=0, tiled=False)
        kvt_all = jnp.swapaxes(kv_all, 2, 3)
        wq = w_query.reshape(d_model, full)
        q = dot(hid, wq, NN).astype(jnp.bfloat16).reshape(n_batch, seq_loc, full)
        do = dot(gout, wo, NT).astype(jnp.bfloat16).reshape(n_batch, seq_loc, full)
        me_arr = me.astype(jnp.int32).reshape(1)

        heads = HEADS_PER_GROUP
        n_groups = n_heads // heads
        dkv, os, dqs, dwo, dwq = None, [], [], [], []
        base = list(range(n_sp))
        for g in range(n_groups):
            o_g, dq_g, dkv = attend(g, heads, me_arr, q, do, kv_all, kvt_all, cos2, sin2, dkv)
            o_g = o_g.reshape(n_rows, heads * head_dim)
            dq_g = dq_g.reshape(n_rows, heads * head_dim)
            os.append(o_g)
            dqs.append(dq_g)
            dwo.append(dot(o_g, gout, (((0,), (0,)), ((), ()))))
            dwq.append(dot(hid, dq_g, (((0,), (0,)), ((), ()))))
            if g < n_groups - 1:
                order = [base[g + 1:] + base[:g + 1]]
                me_arr, dwo[g], dwq[g] = lax.optimization_barrier((me_arr, dwo[g], dwq[g]))
                if g > 0:
                    me_arr, dwo[g - 1], dwq[g - 1] = lax.optimization_barrier((me_arr, dwo[g - 1], dwq[g - 1]))
                dwo[g], dwq[g] = lax.psum((dwo[g], dwq[g]), 'sp', axis_index_groups=order)
        dkv, dwo[-2], dwq[-2] = lax.optimization_barrier((dkv, dwo[-2], dwq[-2]))
        attn_out = dot(jnp.concatenate(os, axis=1), wo, NN).astype(jnp.bfloat16)
        dkv_loc = lax.psum_scatter(dkv, 'sp', scatter_dimension=0, tiled=False)
        dk_f = dkv_loc[..., :head_dim]
        dk_raw = (dk_f * cos2 - swap_halves(dk_f) * sin2).astype(jnp.bfloat16)
        dkv_raw = jnp.concatenate([dk_raw, dkv_loc[..., head_dim:].astype(jnp.bfloat16)], axis=-1).reshape(n_rows, 2 * head_dim)
        dw_kv = dot(hid, dkv_raw, (((0,), (0,)), ((), ())))
        dwo[-1], dwq[-1], dw_kv = lax.psum((dwo[-1], dwq[-1], dw_kv), 'sp')
        d_hidden = (dot(jnp.concatenate(dqs, axis=1), wq, NT) + dot(dkv_raw, w_kv, NT)).astype(jnp.bfloat16)
        dw_query = jnp.concatenate([w.reshape(d_model, heads, head_dim) for w in dwq], axis=1)
        dw_out = jnp.concatenate(dwo, axis=0).reshape(n_heads, head_dim, d_model)
        return (attn_out.reshape(hid_loc.shape), d_hidden.reshape(hid_loc.shape), dw_query, dw_kv[:, :head_dim], dw_kv[:, head_dim:], dw_out)

    act_spec = P('dp', 'sp', None)
    return jax.shard_map(local_step, mesh=mesh, in_specs=(act_spec, act_spec, P(), P(), P(), P()), out_specs=(act_spec, act_spec, P('dp', None, None), P('dp', None), P('dp', None), P('dp', None, None)), check_vma=False)
```

```python
import functools

import jax
import jax.numpy as jnp
from jax import lax
from jax.experimental import pallas as pl
from jax.experimental.pallas import tpu as pltpu
from jax.sharding import PartitionSpec as P

ROPE_BASE = 10000.0
NEG_BIG = -1e30
HEAD_GROUPS = (6, 6, 4)
KEY_SPAN = 2
NT = (((1,), (1,)), ((), ()))
NN = (((1,), (0,)), ((), ()))


def dot(a, b, dims):
    return lax.dot_general(a, b, dims, preferred_element_type=jnp.float32)


def rope_tables(positions, head_dim):
    half_dim = head_dim // 2
    inv_freq = ROPE_BASE ** (-jnp.arange(half_dim, dtype=jnp.float32) * (2.0 / head_dim))
    angles = positions.astype(jnp.float32)[:, None] * inv_freq[None, :]
    cos_t, sin_t = jnp.cos(angles), jnp.sin(angles)
    return jnp.concatenate([cos_t, cos_t], -1), jnp.concatenate([-sin_t, sin_t], -1)


def swap_halves(x):
    half = x.shape[-1] // 2
    return jnp.concatenate([x[..., half:], x[..., :half]], axis=-1)


def attn_kernel(heads, first, last, blk_ref, q_ref, do_ref, kv_ref, cos_ref, sin_ref, *rest):
    rest = list(rest)
    dkv_in_ref = None if first else rest.pop(0)
    o_ref, dq_ref = rest.pop(0), rest.pop(0)
    dkv_refs = [rest.pop(0) for _ in range(2 if last else 1)]
    q_s, do_s, s_s, ot_s, dqt_s, p_s, ds_s, dp_s = rest
    me = blk_ref[0]
    rows, hd = cos_ref.shape
    n_blk = kv_ref.shape[0] // KEY_SPAN
    blk = kv_ref.shape[2]
    keys = KEY_SPAN * blk
    width = heads * rows
    scale = hd ** -0.5
    end = lax.div(me, KEY_SPAN)
    cos2, sin2 = cos_ref[...], sin_ref[...]
    for h in range(heads):
        q_h = q_ref[0, :, h * hd:(h + 1) * hd].astype(jnp.float32) * scale
        q_s[h * rows:(h + 1) * rows, :] = (q_h * cos2 + swap_halves(q_h) * sin2).astype(jnp.bfloat16)
        do_s[h * rows:(h + 1) * rows, :] = do_ref[0, :, h * hd:(h + 1) * hd]

    def k_span(kb):
        return kv_ref[pl.ds(kb * KEY_SPAN, KEY_SPAN), 0, :, :hd].reshape(keys, hd)

    def v_span(kb):
        return kv_ref[pl.ds(kb * KEY_SPAN, KEY_SPAN), 0, :, hd:].reshape(keys, hd)

    def score_block(kb, mask, m8):
        k_blk = k_span(kb)
        out = []
        for h in range(heads):
            s = dot(k_blk, q_s[h * rows:(h + 1) * rows, :], NT)
            if mask is not None:
                s = jnp.where(mask, s, NEG_BIG)
            s_s[kb, :, h * rows:(h + 1) * rows] = s
            out.append(jnp.max(s.reshape(keys // 8, 8, rows), axis=0))
        return jnp.maximum(m8, jnp.concatenate(out, axis=1))

    m8 = lax.fori_loop(0, end, lambda kb, m: score_block(kb, None, m), jnp.full((8, width), NEG_BIG, jnp.float32))
    key_pos = lax.broadcasted_iota(jnp.int32, (keys, rows), 0) + end * keys
    causal = key_pos <= lax.broadcasted_iota(jnp.int32, (keys, rows), 1) + me * rows
    m8 = score_block(end, causal, m8)
    m = jnp.max(m8, axis=0, keepdims=True)

    ot_s[...] = jnp.zeros_like(ot_s)
    dqt_s[...] = jnp.zeros_like(dqt_s)

    def weigh_values(kb):
        vt = v_span(kb).T
        for h in range(heads):
            cols = slice(h * rows, (h + 1) * rows)
            ot_s[:, cols] += dot(vt, p_s[:, cols], NN)

    def value_block(kb, l8):
        weigh_values(jnp.maximum(kb - 1, 0))
        out = []
        for h in range(heads):
            cols = slice(h * rows, (h + 1) * rows)
            e = jnp.exp(s_s[kb, :, cols] - m[:, cols])
            s_s[kb, :, cols] = e
            out.append(jnp.sum(e.reshape(keys // 8, 8, rows), axis=0))
            p_s[:, cols] = e.astype(jnp.bfloat16)
        return l8 + jnp.concatenate(out, axis=1)

    p_s[...] = jnp.zeros_like(p_s)
    ds_s[...] = jnp.zeros_like(ds_s)
    l8 = lax.fori_loop(0, end + 1, value_block, jnp.zeros((8, width), jnp.float32))
    weigh_values(end)
    p_s[...] = jnp.zeros_like(p_s)
    rl = 1.0 / jnp.sum(l8, axis=0, keepdims=True)
    row_dot = []
    for h in range(heads):
        cols = slice(h * rows, (h + 1) * rows)
        o_t = (ot_s[:, cols] * rl[:, cols]).astype(jnp.bfloat16)
        o_ref[0, :, h * hd:(h + 1) * hd] = o_t.T
        do_t = do_ref[0, :, h * hd:(h + 1) * hd].T
        row_dot.append(jnp.sum(do_t.astype(jnp.float32) * o_t.astype(jnp.float32), axis=0, keepdims=True))
    row_dot = jnp.concatenate(row_dot, axis=1)

    def prob_grads(kb):
        v_blk = v_span(kb)
        for h in range(heads):
            cols = slice(h * rows, (h + 1) * rows)
            dp_s[:, cols] = dot(v_blk, do_s[cols, :], NT)

    def put_dkv(kb, dkv):
        dkv = dkv.reshape(KEY_SPAN, blk, 2 * hd)
        if not first:
            dkv = dkv + dkv_in_ref[pl.ds(kb * KEY_SPAN, KEY_SPAN), 0]
        if last:
            odd = lax.rem(me, 2) == 1
            dkv_refs[0][kb, 0] = jnp.where(odd, dkv[1], dkv[0]).astype(jnp.bfloat16)
            dkv_refs[1][kb, 0] = jnp.where(odd, dkv[0], dkv[1]).astype(jnp.bfloat16)
        else:
            dkv_refs[0][pl.ds(kb * KEY_SPAN, KEY_SPAN), 0] = dkv

    def products(kb):
        kt = k_span(kb).T
        for h in range(heads):
            cols = slice(h * rows, (h + 1) * rows)
            dqt_s[:, cols] += dot(kt, ds_s[:, cols], NN)
        put_dkv(kb, jnp.concatenate([dot(ds_s[...], q_s[...], NN), dot(p_s[...], do_s[...], NN)], axis=1))

    def grad_block(kb, _):
        products(jnp.maximum(kb - 1, 0))
        for h in range(heads):
            cols = slice(h * rows, (h + 1) * rows)
            p = s_s[kb, :, cols] * rl[:, cols]
            ds_s[:, cols] = (p * (dp_s[:, cols] - row_dot[:, cols])).astype(jnp.bfloat16)
            p_s[:, cols] = p.astype(jnp.bfloat16)
        prob_grads(jnp.minimum(kb + 1, end))
        return 0

    prob_grads(0)
    lax.fori_loop(0, end + 1, grad_block, 0)
    products(end)

    def zero_block(kb, _):
        for ref in dkv_refs:
            n = ref.shape[0] // n_blk
            ref[pl.ds(kb * n, n)] = jnp.zeros((n, 1, blk, 2 * hd), ref.dtype)
        return 0

    lax.fori_loop(end + 1, n_blk, zero_block, 0)
    for h in range(heads):
        cols = slice(h * rows, (h + 1) * rows)
        g = dqt_s[:, cols].T
        dq_ref[0, :, h * hd:(h + 1) * hd] = ((g * cos2 - swap_halves(g) * sin2) * scale).astype(jnp.bfloat16)


def attend(group, heads, me, q, do, kv, cos2, sin2, dkv, last=False):
    n_batch, rows, _ = q.shape
    n_blk, _, blk, two_hd = kv.shape
    hd = two_hd // 2
    first = dkv is None
    width = heads * hd
    keys = KEY_SPAN * blk
    head_spec = pl.BlockSpec((1, rows, width), lambda b, s: (b, 0, group))
    kv_spec = pl.BlockSpec((n_blk, 1, blk, two_hd), lambda b, s: (0, b, 0, 0))
    half_spec = pl.BlockSpec((n_blk // 2, 1, blk, two_hd), lambda b, s: (0, b, 0, 0))
    tab_spec = pl.BlockSpec((rows, hd), lambda b, s: (0, 0))
    out_spec = pl.BlockSpec((1, rows, width), lambda b, s: (b, 0, 0))
    in_specs = [head_spec, head_spec, kv_spec, tab_spec, tab_spec]
    operands = [me, q, do, kv, cos2, sin2]
    aliases = {}
    if not first:
        in_specs.append(kv_spec)
        operands.append(dkv)
        if not last:
            aliases = {6: 2}
    head_shape = jax.ShapeDtypeStruct((n_batch, rows, width), jnp.bfloat16)
    if last:
        dkv_specs = [half_spec] * 2
        dkv_shapes = [jax.ShapeDtypeStruct((n_blk // 2, n_batch, blk, two_hd), jnp.bfloat16)] * 2
    else:
        dkv_specs = [kv_spec]
        dkv_shapes = [jax.ShapeDtypeStruct((n_blk, n_batch, blk, two_hd), jnp.float32)]
    scores = n_batch * heads * rows * blk * n_blk
    return pl.pallas_call(
        functools.partial(attn_kernel, heads, first, last),
        grid_spec=pltpu.PrefetchScalarGridSpec(
            num_scalar_prefetch=1,
            grid=(n_batch,),
            in_specs=in_specs,
            out_specs=[out_spec, out_spec] + dkv_specs,
            scratch_shapes=[
                pltpu.VMEM((heads * rows, hd), jnp.bfloat16),
                pltpu.VMEM((heads * rows, hd), jnp.bfloat16),
                pltpu.VMEM((n_blk // KEY_SPAN, keys, heads * rows), jnp.float32),
                pltpu.VMEM((hd, heads * rows), jnp.float32),
                pltpu.VMEM((hd, heads * rows), jnp.float32),
                pltpu.VMEM((keys, heads * rows), jnp.bfloat16),
                pltpu.VMEM((keys, heads * rows), jnp.bfloat16),
                pltpu.VMEM((keys, heads * rows), jnp.float32),
            ],
        ),
        out_shape=[head_shape, head_shape] + dkv_shapes,
        input_output_aliases=aliases,
        compiler_params=pltpu.CompilerParams(vmem_limit_bytes=56 * 1024 * 1024),
        cost_estimate=pl.CostEstimate(flops=24 * scores * hd, bytes_accessed=40_000_000, transcendentals=scores),
    )(*operands)


def solution(mesh):
    n_sp = mesh.shape['sp']

    def local_step(hid_loc, gout_loc, w_query, w_key, w_value, w_out):
        n_batch, seq_loc, d_model = hid_loc.shape
        n_heads, head_dim = w_query.shape[1:]
        full = n_heads * head_dim
        n_rows = n_batch * seq_loc
        me = lax.axis_index('sp')
        cos2, sin2 = rope_tables(me * seq_loc + jnp.arange(seq_loc), head_dim)
        w_kv = jnp.concatenate([w_key, w_value], axis=1)
        hid = hid_loc.reshape(n_rows, d_model)
        gout = gout_loc.reshape(n_rows, d_model)
        wo = w_out.reshape(full, d_model)
        kv = dot(hid, w_kv, NN).astype(jnp.bfloat16).reshape(n_batch, seq_loc, 2 * head_dim)
        k_f = kv[..., :head_dim].astype(jnp.float32)
        k_rot = (k_f * cos2 + swap_halves(k_f) * sin2).astype(jnp.bfloat16)
        kv = jnp.concatenate([k_rot, kv[..., head_dim:]], axis=-1)
        kv_all = lax.all_gather(kv, 'sp', axis=0, tiled=False)
        wq = w_query.reshape(d_model, full)
        q = dot(hid, wq, NN).astype(jnp.bfloat16).reshape(n_batch, seq_loc, full)
        do = dot(gout, wo, NT).astype(jnp.bfloat16).reshape(n_batch, seq_loc, full)
        me_arr = me.astype(jnp.int32).reshape(1)

        groups = HEAD_GROUPS
        n_groups = len(groups)
        dkv, os, dqs, dwo, dwq = None, [], [], [], []
        base = list(range(n_sp))
        start = 0
        for g, heads in enumerate(groups):
            last = g == n_groups - 1
            o_g, dq_g, *dkv = attend(start // heads, heads, me_arr, q, do, kv_all, cos2, sin2, dkv, last)
            dkv = dkv if last else dkv[0]
            start += heads
            o_g = o_g.reshape(n_rows, heads * head_dim)
            dq_g = dq_g.reshape(n_rows, heads * head_dim)
            os.append(o_g)
            dqs.append(dq_g)
            dwo.append(dot(o_g, gout, (((0,), (0,)), ((), ()))))
            dwq.append(dot(hid, dq_g, (((0,), (0,)), ((), ()))))
            if not last:
                order = [base[g + 1:] + base[:g + 1]]
                me_arr, dwo[g], dwq[g] = lax.optimization_barrier((me_arr, dwo[g], dwq[g]))
                if g > 0:
                    me_arr, dwo[g - 1], dwq[g - 1] = lax.optimization_barrier((me_arr, dwo[g - 1], dwq[g - 1]))
                dwo[g], dwq[g] = lax.psum((dwo[g], dwq[g]), 'sp', axis_index_groups=order)
        own, other = dkv
        chip = me // 2
        twin = lax.ppermute(other, 'sp', [(i, i ^ 1) for i in base])
        part = (own.astype(jnp.float32) + twin.astype(jnp.float32)).astype(jnp.bfloat16)
        part, os = lax.optimization_barrier((part, os))
        dkv_loc = lax.dynamic_index_in_dim(part, chip, 0, keepdims=False).astype(jnp.float32)
        for far in range(1, n_sp // 2):
            piece = lax.dynamic_index_in_dim(part, jnp.bitwise_xor(chip, far), 0, keepdims=False)
            piece = lax.ppermute(piece, 'sp', [(i, i ^ (2 * far)) for i in base])
            dkv_loc = dkv_loc + piece.astype(jnp.float32)
        attn_out = dot(jnp.concatenate(os, axis=1), wo, NN).astype(jnp.bfloat16)
        attn_out, dkv_loc = lax.optimization_barrier((attn_out, dkv_loc))
        dk_f = dkv_loc[..., :head_dim]
        dk_raw = (dk_f * cos2 - swap_halves(dk_f) * sin2).astype(jnp.bfloat16)
        dkv_raw = jnp.concatenate([dk_raw, dkv_loc[..., head_dim:].astype(jnp.bfloat16)], axis=-1).reshape(n_rows, 2 * head_dim)
        dw_kv = dot(hid, dkv_raw, (((0,), (0,)), ((), ())))
        dwq[-1] = dwq[-1].reshape(d_model, groups[-1], head_dim)
        dw_kv, dwo, dwq = lax.optimization_barrier((dw_kv, dwo, dwq))
        dwo[-1], dwq[-1], dw_kv = lax.psum((dwo[-1], dwq[-1], dw_kv), 'sp')
        d_hidden = (dot(jnp.concatenate(dqs, axis=1), wq, NT) + dot(dkv_raw, w_kv, NT)).astype(jnp.bfloat16)
        dw_query = jnp.zeros(w_query.shape, jnp.float32)
        dw_out = jnp.zeros((full, d_model), jnp.float32)
        start = 0
        for heads, w_q, w_o in zip(groups, dwq, dwo):
            dw_query = lax.dynamic_update_slice(dw_query, w_q.reshape(d_model, heads, head_dim), (0, start, 0))
            dw_out = lax.dynamic_update_slice(dw_out, w_o, (start * head_dim, 0))
            start += heads
        return (attn_out.reshape(hid_loc.shape), d_hidden.reshape(hid_loc.shape), dw_query, dw_kv[:, :head_dim], dw_kv[:, head_dim:], dw_out.reshape(n_heads, head_dim, d_model))

    act_spec = P('dp', 'sp', None)
    return jax.shard_map(local_step, mesh=mesh, in_specs=(act_spec, act_spec, P(), P(), P(), P()), out_specs=(act_spec, act_spec, P('dp', None, None), P('dp', None), P('dp', None), P('dp', None, None)), check_vma=False)
```

```python
import functools

import jax
import jax.numpy as jnp
from jax import lax
from jax.experimental import pallas as pl
from jax.experimental.pallas import tpu as pltpu
from jax.sharding import PartitionSpec as P

ROPE_BASE = 10000.0
NEG_BIG = -1e30
HEAD_GROUPS = (6, 6, 4)
KEY_SPAN = 2
NT = (((1,), (1,)), ((), ()))
NN = (((1,), (0,)), ((), ()))


def dot(a, b, dims):
    return lax.dot_general(a, b, dims, preferred_element_type=jnp.float32)


def rope_tables(positions, head_dim):
    half_dim = head_dim // 2
    inv_freq = ROPE_BASE ** (-jnp.arange(half_dim, dtype=jnp.float32) * (2.0 / head_dim))
    angles = positions.astype(jnp.float32)[:, None] * inv_freq[None, :]
    cos_t, sin_t = jnp.cos(angles), jnp.sin(angles)
    return jnp.concatenate([cos_t, cos_t], -1), jnp.concatenate([-sin_t, sin_t], -1)


def swap_halves(x):
    half = x.shape[-1] // 2
    return jnp.concatenate([x[..., half:], x[..., :half]], axis=-1)


def attn_kernel(heads, first, last, blk_ref, q_ref, do_ref, kv_ref, cos_ref, sin_ref, *rest):
    rest = list(rest)
    dkv_in_ref = None if first else rest.pop(0)
    o_ref, dq_ref = rest.pop(0), rest.pop(0)
    dkv_refs = [rest.pop(0) for _ in range(2 if last else 1)]
    q_s, do_s, s_s, ot_s, dqt_s, p_s, ds_s, dp_s = rest
    me = blk_ref[0]
    rows, hd = cos_ref.shape
    n_blk = kv_ref.shape[0] // KEY_SPAN
    blk = kv_ref.shape[2]
    keys = KEY_SPAN * blk
    width = heads * rows
    scale = hd ** -0.5
    end = lax.div(me, KEY_SPAN)
    cos2, sin2 = cos_ref[...], sin_ref[...]
    for h in range(heads):
        q_h = q_ref[0, :, h * hd:(h + 1) * hd].astype(jnp.float32) * scale
        q_s[h * rows:(h + 1) * rows, :] = (q_h * cos2 + swap_halves(q_h) * sin2).astype(jnp.bfloat16)
        do_s[h * rows:(h + 1) * rows, :] = do_ref[0, :, h * hd:(h + 1) * hd]

    def k_span(kb):
        return kv_ref[pl.ds(kb * KEY_SPAN, KEY_SPAN), 0, :, :hd].reshape(keys, hd)

    def v_span(kb):
        return kv_ref[pl.ds(kb * KEY_SPAN, KEY_SPAN), 0, :, hd:].reshape(keys, hd)

    def score_block(kb, mask, m8):
        k_blk = k_span(kb)
        out = []
        for h in range(heads):
            s = dot(k_blk, q_s[h * rows:(h + 1) * rows, :], NT)
            if mask is not None:
                s = jnp.where(mask, s, NEG_BIG)
            s_s[kb, :, h * rows:(h + 1) * rows] = s
            out.append(jnp.max(s.reshape(keys // 8, 8, rows), axis=0))
        return jnp.maximum(m8, jnp.concatenate(out, axis=1))

    m8 = lax.fori_loop(0, end, lambda kb, m: score_block(kb, None, m), jnp.full((8, width), NEG_BIG, jnp.float32))
    key_pos = lax.broadcasted_iota(jnp.int32, (keys, rows), 0) + end * keys
    causal = key_pos <= lax.broadcasted_iota(jnp.int32, (keys, rows), 1) + me * rows
    m8 = score_block(end, causal, m8)
    m = jnp.max(m8, axis=0, keepdims=True)

    ot_s[...] = jnp.zeros_like(ot_s)
    dqt_s[...] = jnp.zeros_like(dqt_s)

    def weigh_values(kb):
        vt = v_span(kb).T
        for h in range(heads):
            cols = slice(h * rows, (h + 1) * rows)
            ot_s[:, cols] += dot(vt, p_s[:, cols], NN)

    def value_block(kb, l8):
        weigh_values(jnp.maximum(kb - 1, 0))
        out = []
        for h in range(heads):
            cols = slice(h * rows, (h + 1) * rows)
            e = jnp.exp(s_s[kb, :, cols] - m[:, cols])
            s_s[kb, :, cols] = e
            out.append(jnp.sum(e.reshape(keys // 8, 8, rows), axis=0))
            p_s[:, cols] = e.astype(jnp.bfloat16)
        return l8 + jnp.concatenate(out, axis=1)

    p_s[...] = jnp.zeros_like(p_s)
    ds_s[...] = jnp.zeros_like(ds_s)
    l8 = lax.fori_loop(0, end + 1, value_block, jnp.zeros((8, width), jnp.float32))
    weigh_values(end)
    p_s[...] = jnp.zeros_like(p_s)
    rl = 1.0 / jnp.sum(l8, axis=0, keepdims=True)
    row_dot = []
    for h in range(heads):
        cols = slice(h * rows, (h + 1) * rows)
        o_t = (ot_s[:, cols] * rl[:, cols]).astype(jnp.bfloat16)
        o_ref[0, :, h * hd:(h + 1) * hd] = o_t.T
        do_t = do_ref[0, :, h * hd:(h + 1) * hd].T
        row_dot.append(jnp.sum(do_t.astype(jnp.float32) * o_t.astype(jnp.float32), axis=0, keepdims=True))
    row_dot = jnp.concatenate(row_dot, axis=1)

    def prob_grads(kb):
        v_blk = v_span(kb)
        for h in range(heads):
            cols = slice(h * rows, (h + 1) * rows)
            dp_s[:, cols] = dot(v_blk, do_s[cols, :], NT)

    def put_dkv(kb, dkv):
        dkv = dkv.reshape(KEY_SPAN, blk, 2 * hd)
        if not first:
            dkv = dkv + dkv_in_ref[pl.ds(kb * KEY_SPAN, KEY_SPAN), 0]
        if last:
            odd = lax.rem(me, 2) == 1
            dkv_refs[0][kb, 0] = jnp.where(odd, dkv[1], dkv[0]).astype(jnp.bfloat16)
            dkv_refs[1][kb, 0] = jnp.where(odd, dkv[0], dkv[1]).astype(jnp.bfloat16)
        else:
            dkv_refs[0][pl.ds(kb * KEY_SPAN, KEY_SPAN), 0] = dkv

    def products(kb):
        kt = k_span(kb).T
        for h in range(heads):
            cols = slice(h * rows, (h + 1) * rows)
            dqt_s[:, cols] += dot(kt, ds_s[:, cols], NN)
        put_dkv(kb, jnp.concatenate([dot(ds_s[...], q_s[...], NN), dot(p_s[...], do_s[...], NN)], axis=1))

    def grad_block(kb, _):
        products(jnp.maximum(kb - 1, 0))
        for h in range(heads):
            cols = slice(h * rows, (h + 1) * rows)
            p = s_s[kb, :, cols] * rl[:, cols]
            ds_s[:, cols] = (p * (dp_s[:, cols] - row_dot[:, cols])).astype(jnp.bfloat16)
            p_s[:, cols] = p.astype(jnp.bfloat16)
        prob_grads(jnp.minimum(kb + 1, end))
        return 0

    prob_grads(0)
    lax.fori_loop(0, end + 1, grad_block, 0)
    products(end)

    def zero_block(kb, _):
        for ref in dkv_refs:
            n = ref.shape[0] // n_blk
            ref[pl.ds(kb * n, n)] = jnp.zeros((n, 1, blk, 2 * hd), ref.dtype)
        return 0

    lax.fori_loop(end + 1, n_blk, zero_block, 0)
    for h in range(heads):
        cols = slice(h * rows, (h + 1) * rows)
        g = dqt_s[:, cols].T
        dq_ref[0, :, h * hd:(h + 1) * hd] = ((g * cos2 - swap_halves(g) * sin2) * scale).astype(jnp.bfloat16)


def attend(group, heads, me, q, do, kv, cos2, sin2, dkv, last=False):
    n_batch, rows, _ = q.shape
    n_blk, _, blk, two_hd = kv.shape
    hd = two_hd // 2
    first = dkv is None
    width = heads * hd
    keys = KEY_SPAN * blk
    head_spec = pl.BlockSpec((1, rows, width), lambda b, s: (b, 0, group))
    kv_spec = pl.BlockSpec((n_blk, 1, blk, two_hd), lambda b, s: (0, b, 0, 0))
    half_spec = pl.BlockSpec((n_blk // 2, 1, blk, two_hd), lambda b, s: (0, b, 0, 0))
    tab_spec = pl.BlockSpec((rows, hd), lambda b, s: (0, 0))
    out_spec = pl.BlockSpec((1, rows, width), lambda b, s: (b, 0, 0))
    in_specs = [head_spec, head_spec, kv_spec, tab_spec, tab_spec]
    operands = [me, q, do, kv, cos2, sin2]
    aliases = {}
    if not first:
        in_specs.append(kv_spec)
        operands.append(dkv)
        if not last:
            aliases = {6: 2}
    head_shape = jax.ShapeDtypeStruct((n_batch, rows, width), jnp.bfloat16)
    if last:
        dkv_specs = [half_spec] * 2
        dkv_shapes = [jax.ShapeDtypeStruct((n_blk // 2, n_batch, blk, two_hd), jnp.bfloat16)] * 2
    else:
        dkv_specs = [kv_spec]
        dkv_shapes = [jax.ShapeDtypeStruct((n_blk, n_batch, blk, two_hd), jnp.float32)]
    scores = n_batch * heads * rows * blk * n_blk
    return pl.pallas_call(
        functools.partial(attn_kernel, heads, first, last),
        grid_spec=pltpu.PrefetchScalarGridSpec(
            num_scalar_prefetch=1,
            grid=(n_batch,),
            in_specs=in_specs,
            out_specs=[out_spec, out_spec] + dkv_specs,
            scratch_shapes=[
                pltpu.VMEM((heads * rows, hd), jnp.bfloat16),
                pltpu.VMEM((heads * rows, hd), jnp.bfloat16),
                pltpu.VMEM((n_blk // KEY_SPAN, keys, heads * rows), jnp.float32),
                pltpu.VMEM((hd, heads * rows), jnp.float32),
                pltpu.VMEM((hd, heads * rows), jnp.float32),
                pltpu.VMEM((keys, heads * rows), jnp.bfloat16),
                pltpu.VMEM((keys, heads * rows), jnp.bfloat16),
                pltpu.VMEM((keys, heads * rows), jnp.float32),
            ],
        ),
        out_shape=[head_shape, head_shape] + dkv_shapes,
        input_output_aliases=aliases,
        compiler_params=pltpu.CompilerParams(vmem_limit_bytes=56 * 1024 * 1024),
        cost_estimate=pl.CostEstimate(flops=24 * scores * hd, bytes_accessed=40_000_000, transcendentals=scores),
    )(*operands)


def solution(mesh):
    n_sp = mesh.shape['sp']

    def local_step(hid_loc, gout_loc, w_query, w_key, w_value, w_out):
        n_batch, seq_loc, d_model = hid_loc.shape
        n_heads, head_dim = w_query.shape[1:]
        full = n_heads * head_dim
        n_rows = n_batch * seq_loc
        me = lax.axis_index('sp')
        cos2, sin2 = rope_tables(me * seq_loc + jnp.arange(seq_loc), head_dim)
        base = list(range(n_sp))
        core, chip, n_chip = me % 2, me // 2, n_sp // 2

        def to_twin(x):
            return lax.ppermute(x, 'sp', [(i, i ^ 1) for i in base])

        def to_chip(x, far):
            return lax.ppermute(x, 'sp', [(i, i ^ (2 * far)) for i in base])

        def pick(x, i):
            return lax.dynamic_index_in_dim(x, i, 0, keepdims=False)

        def sum_small(x):
            parts = x.reshape(2, n_chip, x.shape[0] // n_sp, x.shape[1])
            held = pick(parts, core) + to_twin(pick(parts, 1 - core))
            total = pick(held, chip)
            for far in range(1, n_chip):
                total = total + to_chip(pick(held, jnp.bitwise_xor(chip, far)), far)
            half = lax.dynamic_update_index_in_dim(jnp.zeros_like(held), total, chip, 0)
            for far in range(1, n_chip):
                half = lax.dynamic_update_index_in_dim(half, to_chip(total, far), jnp.bitwise_xor(chip, far), 0)
            rest = to_twin(half)
            first, second = jnp.where(core == 0, half, rest), jnp.where(core == 0, rest, half)
            return jnp.concatenate([first, second], axis=0).reshape(x.shape)

        w_kv = jnp.concatenate([w_key, w_value], axis=1)
        hid = hid_loc.reshape(n_rows, d_model)
        gout = gout_loc.reshape(n_rows, d_model)
        wo = w_out.reshape(full, d_model)
        kv = dot(hid, w_kv, NN).astype(jnp.bfloat16).reshape(n_batch, seq_loc, 2 * head_dim)
        k_f = kv[..., :head_dim].astype(jnp.float32)
        k_rot = (k_f * cos2 + swap_halves(k_f) * sin2).astype(jnp.bfloat16)
        kv = jnp.concatenate([k_rot, kv[..., head_dim:]], axis=-1)
        kv_all = lax.all_gather(kv, 'sp', axis=0, tiled=False)
        wq = w_query.reshape(d_model, full)
        q = dot(hid, wq, NN).astype(jnp.bfloat16).reshape(n_batch, seq_loc, full)
        do = dot(gout, wo, NT).astype(jnp.bfloat16).reshape(n_batch, seq_loc, full)
        me_arr = me.astype(jnp.int32).reshape(1)

        groups = HEAD_GROUPS
        n_groups = len(groups)
        dkv, os, dqs, dwo, dwq = None, [], [], [], []
        start = 0
        for g, heads in enumerate(groups):
            last = g == n_groups - 1
            o_g, dq_g, *dkv = attend(start // heads, heads, me_arr, q, do, kv_all, cos2, sin2, dkv, last)
            dkv = dkv if last else dkv[0]
            start += heads
            o_g = o_g.reshape(n_rows, heads * head_dim)
            dq_g = dq_g.reshape(n_rows, heads * head_dim)
            os.append(o_g)
            dqs.append(dq_g)
            dwo.append(dot(o_g, gout, (((0,), (0,)), ((), ()))))
            dwq.append(dot(hid, dq_g, (((0,), (0,)), ((), ()))))
            order = [base[g + 1:] + base[:g + 1]]
            if last:
                dwq[g] = dwq[g].reshape(d_model, heads, head_dim)
                dwo[g], dwq[g] = lax.psum((dwo[g], dwq[g]), 'sp', axis_index_groups=order)
            else:
                me_arr, dwo[g], dwq[g] = lax.optimization_barrier((me_arr, dwo[g], dwq[g]))
                if g > 0:
                    me_arr, dwo[g - 1], dwq[g - 1] = lax.optimization_barrier((me_arr, dwo[g - 1], dwq[g - 1]))
                dwo[g], dwq[g] = lax.psum((dwo[g], dwq[g]), 'sp', axis_index_groups=order)
        own, other = dkv
        part = (own.astype(jnp.float32) + to_twin(other).astype(jnp.float32)).astype(jnp.bfloat16)
        part, os = lax.optimization_barrier((part, os))
        dkv_loc = pick(part, chip).astype(jnp.float32)
        for far in range(1, n_chip):
            dkv_loc = dkv_loc + to_chip(pick(part, jnp.bitwise_xor(chip, far)), far).astype(jnp.float32)
        attn_out = dot(jnp.concatenate(os, axis=1), wo, NN).astype(jnp.bfloat16)
        attn_out, dkv_loc = lax.optimization_barrier((attn_out, dkv_loc))
        dk_f = dkv_loc[..., :head_dim]
        dk_raw = (dk_f * cos2 - swap_halves(dk_f) * sin2).astype(jnp.bfloat16)
        dkv_raw = jnp.concatenate([dk_raw, dkv_loc[..., head_dim:].astype(jnp.bfloat16)], axis=-1).reshape(n_rows, 2 * head_dim)
        dw_kv = dot(hid, dkv_raw, (((0,), (0,)), ((), ())))
        dw_kv = sum_small(dw_kv)
        d_hidden = (dot(jnp.concatenate(dqs, axis=1), wq, NT) + dot(dkv_raw, w_kv, NT)).astype(jnp.bfloat16)
        done = n_heads - groups[-1]
        dwq = [w.reshape(d_model, heads, head_dim) for heads, w in zip(groups, dwq)]
        dw_query = jnp.concatenate(dwq[:-1] + [jnp.zeros((d_model, groups[-1], head_dim), jnp.float32)], axis=1)
        dw_query = lax.dynamic_update_slice(dw_query, dwq[-1], (0, done, 0))
        dw_out = jnp.concatenate(dwo[:-1] + [jnp.zeros((groups[-1] * head_dim, d_model), jnp.float32)], axis=0)
        dw_out = lax.dynamic_update_slice(dw_out, dwo[-1], (done * head_dim, 0))
        return (attn_out.reshape(hid_loc.shape), d_hidden.reshape(hid_loc.shape), dw_query, dw_kv[:, :head_dim], dw_kv[:, head_dim:], dw_out.reshape(n_heads, head_dim, d_model))

    act_spec = P('dp', 'sp', None)
    return jax.shard_map(local_step, mesh=mesh, in_specs=(act_spec, act_spec, P(), P(), P(), P()), out_specs=(act_spec, act_spec, P('dp', None, None), P('dp', None), P('dp', None), P('dp', None, None)), check_vma=False)
```

```python
import functools

import jax
import jax.numpy as jnp
from jax import lax
from jax.experimental import pallas as pl
from jax.experimental.pallas import tpu as pltpu
from jax.sharding import PartitionSpec as P

ROPE_BASE = 10000.0
NEG_BIG = -1e30
HEAD_GROUPS = ((12, 4), (6, 6), (0, 6))
KEY_SPAN = 2
NT = (((1,), (1,)), ((), ()))
NN = (((1,), (0,)), ((), ()))


def dot(a, b, dims):
    return lax.dot_general(a, b, dims, preferred_element_type=jnp.float32)


def rope_tables(positions, head_dim):
    half_dim = head_dim // 2
    inv_freq = ROPE_BASE ** (-jnp.arange(half_dim, dtype=jnp.float32) * (2.0 / head_dim))
    angles = positions.astype(jnp.float32)[:, None] * inv_freq[None, :]
    cos_t, sin_t = jnp.cos(angles), jnp.sin(angles)
    return jnp.concatenate([cos_t, cos_t], -1), jnp.concatenate([-sin_t, sin_t], -1)


def swap_halves(x):
    half = x.shape[-1] // 2
    return jnp.concatenate([x[..., half:], x[..., :half]], axis=-1)


def attn_kernel(heads, first, last, blk_ref, q_ref, do_ref, kv_ref, cos_ref, sin_ref, *rest):
    rest = list(rest)
    dkv_in_ref = None if first else rest.pop(0)
    o_ref, dq_ref = rest.pop(0), rest.pop(0)
    dkv_refs = [rest.pop(0) for _ in range(2 if last else 1)]
    q_s, do_s, s_s, ot_s, dqt_s, p_s, ds_s, dp_s = rest
    me = blk_ref[0]
    rows, hd = cos_ref.shape
    n_blk = kv_ref.shape[0] // KEY_SPAN
    blk = kv_ref.shape[2]
    keys = KEY_SPAN * blk
    width = heads * rows
    scale = hd ** -0.5
    end = lax.div(me, KEY_SPAN)
    cos2, sin2 = cos_ref[...], sin_ref[...]
    for h in range(heads):
        q_h = q_ref[0, :, h * hd:(h + 1) * hd].astype(jnp.float32) * scale
        q_s[h * rows:(h + 1) * rows, :] = (q_h * cos2 + swap_halves(q_h) * sin2).astype(jnp.bfloat16)
        do_s[h * rows:(h + 1) * rows, :] = do_ref[0, :, h * hd:(h + 1) * hd]

    def k_span(kb):
        return kv_ref[pl.ds(kb * KEY_SPAN, KEY_SPAN), 0, :, :hd].reshape(keys, hd)

    def v_span(kb):
        return kv_ref[pl.ds(kb * KEY_SPAN, KEY_SPAN), 0, :, hd:].reshape(keys, hd)

    def score_block(kb, mask, m8):
        k_blk = k_span(kb)
        out = []
        for h in range(heads):
            s = dot(k_blk, q_s[h * rows:(h + 1) * rows, :], NT)
            if mask is not None:
                s = jnp.where(mask, s, NEG_BIG)
            s_s[kb, :, h * rows:(h + 1) * rows] = s
            out.append(jnp.max(s.reshape(keys // 8, 8, rows), axis=0))
        return jnp.maximum(m8, jnp.concatenate(out, axis=1))

    m8 = lax.fori_loop(0, end, lambda kb, m: score_block(kb, None, m), jnp.full((8, width), NEG_BIG, jnp.float32))
    key_pos = lax.broadcasted_iota(jnp.int32, (keys, rows), 0) + end * keys
    causal = key_pos <= lax.broadcasted_iota(jnp.int32, (keys, rows), 1) + me * rows
    m8 = score_block(end, causal, m8)
    m = jnp.max(m8, axis=0, keepdims=True)

    ot_s[...] = jnp.zeros_like(ot_s)
    dqt_s[...] = jnp.zeros_like(dqt_s)

    def weigh_values(kb):
        vt = v_span(kb).T
        for h in range(heads):
            cols = slice(h * rows, (h + 1) * rows)
            ot_s[:, cols] += dot(vt, p_s[:, cols], NN)

    def value_block(kb, l8):
        weigh_values(jnp.maximum(kb - 1, 0))
        out = []
        for h in range(heads):
            cols = slice(h * rows, (h + 1) * rows)
            e = jnp.exp(s_s[kb, :, cols] - m[:, cols])
            s_s[kb, :, cols] = e
            out.append(jnp.sum(e.reshape(keys // 8, 8, rows), axis=0))
            p_s[:, cols] = e.astype(jnp.bfloat16)
        return l8 + jnp.concatenate(out, axis=1)

    p_s[...] = jnp.zeros_like(p_s)
    ds_s[...] = jnp.zeros_like(ds_s)
    l8 = lax.fori_loop(0, end + 1, value_block, jnp.zeros((8, width), jnp.float32))
    weigh_values(end)
    p_s[...] = jnp.zeros_like(p_s)
    rl = 1.0 / jnp.sum(l8, axis=0, keepdims=True)
    row_dot = []
    for h in range(heads):
        cols = slice(h * rows, (h + 1) * rows)
        o_t = (ot_s[:, cols] * rl[:, cols]).astype(jnp.bfloat16)
        o_ref[0, :, h * hd:(h + 1) * hd] = o_t.T
        do_t = do_ref[0, :, h * hd:(h + 1) * hd].T
        row_dot.append(jnp.sum(do_t.astype(jnp.float32) * o_t.astype(jnp.float32), axis=0, keepdims=True))
    row_dot = jnp.concatenate(row_dot, axis=1)

    def prob_grads(kb):
        v_blk = v_span(kb)
        for h in range(heads):
            cols = slice(h * rows, (h + 1) * rows)
            dp_s[:, cols] = dot(v_blk, do_s[cols, :], NT)

    def put_dkv(kb, dkv):
        dkv = dkv.reshape(KEY_SPAN, blk, 2 * hd)
        if not first:
            dkv = dkv + dkv_in_ref[pl.ds(kb * KEY_SPAN, KEY_SPAN), 0]
        if last:
            odd = lax.rem(me, 2) == 1
            dkv_refs[0][kb, 0] = jnp.where(odd, dkv[1], dkv[0]).astype(jnp.bfloat16)
            dkv_refs[1][kb, 0] = jnp.where(odd, dkv[0], dkv[1]).astype(jnp.bfloat16)
        else:
            dkv_refs[0][pl.ds(kb * KEY_SPAN, KEY_SPAN), 0] = dkv

    def products(kb):
        kt = k_span(kb).T
        for h in range(heads):
            cols = slice(h * rows, (h + 1) * rows)
            dqt_s[:, cols] += dot(kt, ds_s[:, cols], NN)
        put_dkv(kb, jnp.concatenate([dot(ds_s[...], q_s[...], NN), dot(p_s[...], do_s[...], NN)], axis=1))

    def grad_block(kb, _):
        products(jnp.maximum(kb - 1, 0))
        for h in range(heads):
            cols = slice(h * rows, (h + 1) * rows)
            p = s_s[kb, :, cols] * rl[:, cols]
            ds_s[:, cols] = (p * (dp_s[:, cols] - row_dot[:, cols])).astype(jnp.bfloat16)
            p_s[:, cols] = p.astype(jnp.bfloat16)
        prob_grads(jnp.minimum(kb + 1, end))
        return 0

    prob_grads(0)
    lax.fori_loop(0, end + 1, grad_block, 0)
    products(end)

    def zero_block(kb, _):
        for ref in dkv_refs:
            n = ref.shape[0] // n_blk
            ref[pl.ds(kb * n, n)] = jnp.zeros((n, 1, blk, 2 * hd), ref.dtype)
        return 0

    lax.fori_loop(end + 1, n_blk, zero_block, 0)
    for h in range(heads):
        cols = slice(h * rows, (h + 1) * rows)
        g = dqt_s[:, cols].T
        dq_ref[0, :, h * hd:(h + 1) * hd] = ((g * cos2 - swap_halves(g) * sin2) * scale).astype(jnp.bfloat16)


def attend(group, heads, me, q, do, kv, cos2, sin2, dkv, last=False):
    n_batch, rows, _ = q.shape
    n_blk, _, blk, two_hd = kv.shape
    hd = two_hd // 2
    first = dkv is None
    width = heads * hd
    keys = KEY_SPAN * blk
    head_spec = pl.BlockSpec((1, rows, width), lambda b, s: (b, 0, group))
    kv_spec = pl.BlockSpec((n_blk, 1, blk, two_hd), lambda b, s: (0, b, 0, 0))
    half_spec = pl.BlockSpec((n_blk // 2, 1, blk, two_hd), lambda b, s: (0, b, 0, 0))
    tab_spec = pl.BlockSpec((rows, hd), lambda b, s: (0, 0))
    out_spec = pl.BlockSpec((1, rows, width), lambda b, s: (b, 0, 0))
    in_specs = [head_spec, head_spec, kv_spec, tab_spec, tab_spec]
    operands = [me, q, do, kv, cos2, sin2]
    aliases = {}
    if not first:
        in_specs.append(kv_spec)
        operands.append(dkv)
        if not last:
            aliases = {6: 2}
    head_shape = jax.ShapeDtypeStruct((n_batch, rows, width), jnp.bfloat16)
    if last:
        dkv_specs = [half_spec] * 2
        dkv_shapes = [jax.ShapeDtypeStruct((n_blk // 2, n_batch, blk, two_hd), jnp.bfloat16)] * 2
    else:
        dkv_specs = [kv_spec]
        dkv_shapes = [jax.ShapeDtypeStruct((n_blk, n_batch, blk, two_hd), jnp.float32)]
    scores = n_batch * heads * rows * blk * n_blk
    return pl.pallas_call(
        functools.partial(attn_kernel, heads, first, last),
        grid_spec=pltpu.PrefetchScalarGridSpec(
            num_scalar_prefetch=1,
            grid=(n_batch,),
            in_specs=in_specs,
            out_specs=[out_spec, out_spec] + dkv_specs,
            scratch_shapes=[
                pltpu.VMEM((heads * rows, hd), jnp.bfloat16),
                pltpu.VMEM((heads * rows, hd), jnp.bfloat16),
                pltpu.VMEM((n_blk // KEY_SPAN, keys, heads * rows), jnp.float32),
                pltpu.VMEM((hd, heads * rows), jnp.float32),
                pltpu.VMEM((hd, heads * rows), jnp.float32),
                pltpu.VMEM((keys, heads * rows), jnp.bfloat16),
                pltpu.VMEM((keys, heads * rows), jnp.bfloat16),
                pltpu.VMEM((keys, heads * rows), jnp.float32),
            ],
        ),
        out_shape=[head_shape, head_shape] + dkv_shapes,
        input_output_aliases=aliases,
        compiler_params=pltpu.CompilerParams(vmem_limit_bytes=56 * 1024 * 1024),
        cost_estimate=pl.CostEstimate(flops=24 * scores * hd, bytes_accessed=40_000_000, transcendentals=scores),
    )(*operands)


def solution(mesh):
    n_sp = mesh.shape['sp']

    def local_step(hid_loc, gout_loc, w_query, w_key, w_value, w_out):
        n_batch, seq_loc, d_model = hid_loc.shape
        n_heads, head_dim = w_query.shape[1:]
        full = n_heads * head_dim
        n_rows = n_batch * seq_loc
        me = lax.axis_index('sp')
        cos2, sin2 = rope_tables(me * seq_loc + jnp.arange(seq_loc), head_dim)
        base = list(range(n_sp))
        core, chip, n_chip = me % 2, me // 2, n_sp // 2

        def to_twin(x):
            return lax.ppermute(x, 'sp', [(i, i ^ 1) for i in base])

        def to_chip(x, far):
            return lax.ppermute(x, 'sp', [(i, i ^ (2 * far)) for i in base])

        def to_lower_chip(x, far):
            return lax.ppermute(x, 'sp', [(i, i ^ (2 * far)) for i in base if i ^ (2 * far) < i])

        def pick(x, i):
            return lax.dynamic_index_in_dim(x, i, 0, keepdims=False)

        def sum_small(x):
            parts = x.reshape(2, n_chip, x.shape[0] // n_sp, x.shape[1])
            held = pick(parts, core) + to_twin(pick(parts, 1 - core))
            total = pick(held, chip)
            for far in range(1, n_chip):
                total = total + to_chip(pick(held, jnp.bitwise_xor(chip, far)), far)
            half = lax.dynamic_update_index_in_dim(jnp.zeros_like(held), total, chip, 0)
            for far in range(1, n_chip):
                half = lax.dynamic_update_index_in_dim(half, to_chip(total, far), jnp.bitwise_xor(chip, far), 0)
            rest = to_twin(half)
            first, second = jnp.where(core == 0, half, rest), jnp.where(core == 0, rest, half)
            return jnp.concatenate([first, second], axis=0).reshape(x.shape)

        w_kv = jnp.concatenate([w_key, w_value], axis=1)
        hid = hid_loc.reshape(n_rows, d_model)
        gout = gout_loc.reshape(n_rows, d_model)
        wo = w_out.reshape(full, d_model)
        kv = dot(hid, w_kv, NN).astype(jnp.bfloat16).reshape(n_batch, seq_loc, 2 * head_dim)
        k_f = kv[..., :head_dim].astype(jnp.float32)
        k_rot = (k_f * cos2 + swap_halves(k_f) * sin2).astype(jnp.bfloat16)
        kv = jnp.concatenate([k_rot, kv[..., head_dim:]], axis=-1)
        kv_all = lax.all_gather(kv, 'sp', axis=0, tiled=False)
        wq = w_query.reshape(d_model, full)
        q = dot(hid, wq, NN).astype(jnp.bfloat16).reshape(n_batch, seq_loc, full)
        do = dot(gout, wo, NT).astype(jnp.bfloat16).reshape(n_batch, seq_loc, full)
        me_arr = me.astype(jnp.int32).reshape(1)

        groups = HEAD_GROUPS
        n_groups = len(groups)
        dkv, os, dqs, dwo, dwq = None, [], [], [], []
        for g, (start, heads) in enumerate(groups):
            last = g == n_groups - 1
            o_g, dq_g, *dkv = attend(start // heads, heads, me_arr, q, do, kv_all, cos2, sin2, dkv, last)
            dkv = dkv if last else dkv[0]
            o_g = o_g.reshape(n_rows, heads * head_dim)
            dq_g = dq_g.reshape(n_rows, heads * head_dim)
            os.append(o_g)
            dqs.append(dq_g)
            dwo.append(dot(o_g, gout, (((0,), (0,)), ((), ()))))
            dwq.append(dot(hid, dq_g, (((0,), (0,)), ((), ()))))
            order = [base[g + 1:] + base[:g + 1]]
            if last:
                dwq[g] = dwq[g].reshape(d_model, heads, head_dim)
                dwo[g], dwq[g] = lax.psum((dwo[g], dwq[g]), 'sp', axis_index_groups=order)
            else:
                me_arr, dwo[g], dwq[g] = lax.optimization_barrier((me_arr, dwo[g], dwq[g]))
                if g > 0:
                    me_arr, dwo[g - 1], dwq[g - 1] = lax.optimization_barrier((me_arr, dwo[g - 1], dwq[g - 1]))
                dwo[g], dwq[g] = lax.psum((dwo[g], dwq[g]), 'sp', axis_index_groups=order)
                dwo[g], dwq[g] = lax.optimization_barrier((dwo[g], dwq[g]))

        def by_head(pieces):
            return [piece for _, piece in sorted(zip([start for start, _ in groups], pieces), key=lambda pair: pair[0])]

        own, other = dkv
        part = (own.astype(jnp.float32) + to_twin(other).astype(jnp.float32)).astype(jnp.bfloat16)
        part, os = lax.optimization_barrier((part, os))
        dkv_loc = pick(part, chip).astype(jnp.float32)
        for far in range(1, n_chip):
            dkv_loc = dkv_loc + to_lower_chip(pick(part, jnp.bitwise_xor(chip, far)), far).astype(jnp.float32)
        attn_out = dot(jnp.concatenate(by_head(os), axis=1), wo, NN).astype(jnp.bfloat16)
        attn_out, dkv_loc = lax.optimization_barrier((attn_out, dkv_loc))
        dk_f = dkv_loc[..., :head_dim]
        dk_raw = (dk_f * cos2 - swap_halves(dk_f) * sin2).astype(jnp.bfloat16)
        dkv_raw = jnp.concatenate([dk_raw, dkv_loc[..., head_dim:].astype(jnp.bfloat16)], axis=-1).reshape(n_rows, 2 * head_dim)
        dw_kv = dot(hid, dkv_raw, (((0,), (0,)), ((), ())))
        dw_kv = sum_small(dw_kv)
        d_hidden = (dot(jnp.concatenate(by_head(dqs), axis=1), wq, NT) + dot(dkv_raw, w_kv, NT)).astype(jnp.bfloat16)
        start, heads = groups[-1]
        dwq = [w.reshape(d_model, n, head_dim) for (_, n), w in zip(groups, dwq)]
        dw_query = jnp.concatenate(by_head(dwq[:-1] + [jnp.zeros((d_model, heads, head_dim), jnp.float32)]), axis=1)
        dw_query = lax.dynamic_update_slice(dw_query, dwq[-1], (0, start, 0))
        dw_out = jnp.concatenate(by_head(dwo[:-1] + [jnp.zeros((heads * head_dim, d_model), jnp.float32)]), axis=0)
        dw_out = lax.dynamic_update_slice(dw_out, dwo[-1], (start * head_dim, 0))
        return (attn_out.reshape(hid_loc.shape), d_hidden.reshape(hid_loc.shape), dw_query, dw_kv[:, :head_dim], dw_kv[:, head_dim:], dw_out.reshape(n_heads, head_dim, d_model))

    act_spec = P('dp', 'sp', None)
    return jax.shard_map(local_step, mesh=mesh, in_specs=(act_spec, act_spec, P(), P(), P(), P()), out_specs=(act_spec, act_spec, P('dp', None, None), P('dp', None), P('dp', None), P('dp', None, None)), check_vma=False)
```
